8 devices in a mesh: data: 2 (over z, y), dap: 4 (over x, core).
Axes of the slice: x: 2, y: 2, z: 1, core: 2. Of those that a mesh axis runs over, the one named last changes fastest.
Arguments:
- pair_act: float32 [768, 384, 128], P(('data', 'dap')), parts along dimension 0
- pair_mask: int32 [768, 384], P(('data', 'dap')), parts along dimension 0
- msa_act: bfloat16 [512, 768, 256], P(None, ('data', 'dap')), parts along dimension 1
- opm_norm: float32 [2, 256], replicated
- opm_proj: bfloat16 [256, 64], replicated
- opm_out: bfloat16 [1024, 128], replicated
- opm_bias: float32 [128], replicated
- tri_norm: float32 [2, 2, 128], replicated
- tri_proj: bfloat16 [2, 128, 512], replicated
- tri_gate: bfloat16 [2, 128, 128], replicated
- tri_xnorm: float32 [2, 2, 128], replicated
- tri_out: bfloat16 [2, 128, 128], replicated
Outputs:
- output: float32 [768, 384, 128], P(('data', 'dap')), parts along dimension 0
There are 2 independent parts. The reference program is written for one: setup_inputs(seed, part) draws one part's arguments, and reference() takes and returns one part's arrays. A program takes and returns all parts, laid end to end along the dimension named above; an argument that names none is the same for every part.
All inputs are finite; a program needn't handle non-finite values.
Results may differ from the reference program's by a relative error of at most 0.00319395.
Values are sent between devices in bfloat16 or wider.
A program may use at most 1 GiB of HBM per device.

```python
import jax
import jax.numpy as jnp
from jax import lax

RESIDUES = 384
PAIR_DIM = 128
TRI_DIM = 128
MSA_DIM = 256
OPM_DIM = 32
MSA_DEPTH = 512
ROW_BLOCK = 32
NUM_BLOCKS = RESIDUES // ROW_BLOCK
LN_EPS = 1e-5


def layer_norm(values, norm_scale, norm_shift):
    row_mean = jnp.mean(values, axis=-1, keepdims=True)
    centered = values - row_mean
    row_var = jnp.mean(centered * centered, axis=-1, keepdims=True)
    return (centered * lax.rsqrt(row_var + LN_EPS) * norm_scale + norm_shift).astype(jnp.bfloat16)


def outer_product_mean(msa_act, opm_norm, opm_proj, opm_out, opm_bias):
    msa_norm = layer_norm(msa_act.astype(jnp.float32), opm_norm[0], opm_norm[1])
    proj_all = jnp.dot(msa_norm.reshape(MSA_DEPTH * RESIDUES, MSA_DIM), opm_proj, preferred_element_type=jnp.float32)
    proj_all = proj_all.astype(jnp.bfloat16).reshape(MSA_DEPTH, RESIDUES, 2 * OPM_DIM)
    left_proj = proj_all[:, :, :OPM_DIM].astype(jnp.float32)
    right_proj = proj_all[:, :, OPM_DIM:].astype(jnp.float32)
    left_blocks = jnp.moveaxis(left_proj.reshape(MSA_DEPTH, NUM_BLOCKS, ROW_BLOCK, OPM_DIM), 1, 0)

    def block_update(left_blk):
        outer_prod = jnp.einsum("sip,sjq->ijpq", left_blk, right_proj) / MSA_DEPTH
        outer_flat = outer_prod.astype(jnp.bfloat16).reshape(ROW_BLOCK * RESIDUES, OPM_DIM * OPM_DIM)
        return jnp.dot(outer_flat, opm_out, preferred_element_type=jnp.float32).reshape(ROW_BLOCK, RESIDUES, PAIR_DIM)

    opm_update = lax.map(block_update, left_blocks).reshape(RESIDUES, RESIDUES, PAIR_DIM)
    return opm_update + opm_bias


def triangle_update(pair_act, mask_f, norm_pair, w_proj, w_gate, norm_mix, w_out, incoming):
    pair_blocks = pair_act.reshape(NUM_BLOCKS, ROW_BLOCK, RESIDUES, PAIR_DIM)
    mask_blocks = mask_f.reshape(NUM_BLOCKS, ROW_BLOCK, RESIDUES, 1)

    def project(blk_args):
        pair_blk, mask_blk = blk_args
        pair_norm = layer_norm(pair_blk, norm_pair[0], norm_pair[1])
        proj_all = jnp.dot(pair_norm.reshape(ROW_BLOCK * RESIDUES, PAIR_DIM), w_proj, preferred_element_type=jnp.float32)
        proj_all = proj_all.reshape(ROW_BLOCK, RESIDUES, 4 * TRI_DIM)
        left_act = mask_blk * jax.nn.sigmoid(proj_all[:, :, TRI_DIM:2 * TRI_DIM]) * proj_all[:, :, :TRI_DIM]
        right_act = mask_blk * jax.nn.sigmoid(proj_all[:, :, 3 * TRI_DIM:]) * proj_all[:, :, 2 * TRI_DIM:3 * TRI_DIM]
        return left_act.astype(jnp.bfloat16), right_act.astype(jnp.bfloat16)

    left_all, right_all = lax.map(project, (pair_blocks, mask_blocks))
    left_all = left_all.reshape(RESIDUES, RESIDUES, TRI_DIM)
    right_all = right_all.reshape(RESIDUES, RESIDUES, TRI_DIM)
    if incoming:
        left_all = jnp.swapaxes(left_all, 0, 1)
        right_all = jnp.swapaxes(right_all, 0, 1)
    right_wide = right_all.astype(jnp.float32)
    left_blocks = left_all.reshape(NUM_BLOCKS, ROW_BLOCK, RESIDUES, TRI_DIM)

    def combine(blk_args):
        pair_blk, left_blk = blk_args
        mixed_act = jnp.einsum("ikc,jkc->ijc", left_blk.astype(jnp.float32), right_wide).astype(jnp.bfloat16)
        mixed_norm = layer_norm(mixed_act.astype(jnp.float32), norm_mix[0], norm_mix[1])
        update = jnp.dot(mixed_norm.reshape(ROW_BLOCK * RESIDUES, TRI_DIM), w_out, preferred_element_type=jnp.float32)
        pair_norm = layer_norm(pair_blk, norm_pair[0], norm_pair[1])
        gate_act = jax.nn.sigmoid(jnp.dot(pair_norm.reshape(ROW_BLOCK * RESIDUES, PAIR_DIM), w_gate, preferred_element_type=jnp.float32))
        return pair_blk + (gate_act * update).reshape(ROW_BLOCK, RESIDUES, PAIR_DIM)

    return lax.map(combine, (pair_blocks, left_blocks)).reshape(RESIDUES, RESIDUES, PAIR_DIM)


def setup_inputs(seed: int = 0, part: int = 0) -> dict:
    part_keys = jax.random.split(jax.random.fold_in(jax.random.key(seed), part), 5)
    shared_keys = jax.random.split(jax.random.key(seed + 1), 12)

    def scaled_normal(key_w, shape_w, fan_in):
        return (jax.random.normal(key_w, shape_w, jnp.float32) * fan_in ** -0.5).astype(jnp.bfloat16)

    pair_act = jax.random.normal(part_keys[0], (RESIDUES, RESIDUES, PAIR_DIM), jnp.float32)
    valid_len = jax.random.randint(part_keys[1], (), RESIDUES - RESIDUES // 8, RESIDUES - RESIDUES // 32 + 1)
    positions = jnp.arange(RESIDUES)
    in_range = positions < valid_len
    kept_entries = jax.random.randint(part_keys[2], (RESIDUES, RESIDUES), 0, 32) != 0
    pair_mask = (in_range[:, None] & in_range[None, :] & kept_entries).astype(jnp.int32)
    profile = jax.random.normal(part_keys[3], (RESIDUES, MSA_DIM), jnp.float32)
    msa_noise = jax.random.normal(part_keys[4], (MSA_DEPTH, RESIDUES, MSA_DIM), jnp.float32)
    msa_act = (profile[None] + 0.75 * msa_noise).astype(jnp.bfloat16)
    opm_norm = jnp.stack([1.0 + 0.3 * jax.random.normal(shared_keys[0], (MSA_DIM,), jnp.float32), 0.3 * jax.random.normal(shared_keys[1], (MSA_DIM,), jnp.float32)])
    opm_proj = scaled_normal(shared_keys[2], (MSA_DIM, 2 * OPM_DIM), MSA_DIM)
    opm_out = scaled_normal(shared_keys[3], (OPM_DIM * OPM_DIM, PAIR_DIM), OPM_DIM * OPM_DIM)
    opm_bias = 0.5 * jax.random.normal(shared_keys[4], (PAIR_DIM,), jnp.float32)
    tri_norm = jnp.concatenate([1.0 + 0.3 * jax.random.normal(shared_keys[5], (2, 1, PAIR_DIM), jnp.float32), 0.3 * jax.random.normal(shared_keys[6], (2, 1, PAIR_DIM), jnp.float32)], axis=1)
    tri_proj = scaled_normal(shared_keys[7], (2, PAIR_DIM, 4 * TRI_DIM), PAIR_DIM)
    tri_gate = scaled_normal(shared_keys[8], (2, PAIR_DIM, PAIR_DIM), PAIR_DIM)
    tri_xnorm = jnp.concatenate([1.0 + 0.3 * jax.random.normal(shared_keys[9], (2, 1, TRI_DIM), jnp.float32), 0.3 * jax.random.normal(shared_keys[10], (2, 1, TRI_DIM), jnp.float32)], axis=1)
    tri_out = scaled_normal(shared_keys[11], (2, TRI_DIM, PAIR_DIM), TRI_DIM)
    return {"pair_act": pair_act, "pair_mask": pair_mask, "msa_act": msa_act, "opm_norm": opm_norm, "opm_proj": opm_proj, "opm_out": opm_out, "opm_bias": opm_bias, "tri_norm": tri_norm, "tri_proj": tri_proj, "tri_gate": tri_gate, "tri_xnorm": tri_xnorm, "tri_out": tri_out}


def reference(pair_act, pair_mask, msa_act, opm_norm, opm_proj, opm_out, opm_bias, tri_norm, tri_proj, tri_gate, tri_xnorm, tri_out):
    mask_f = pair_mask.astype(jnp.float32)
    pair_zero = pair_act + outer_product_mean(msa_act, opm_norm, opm_proj, opm_out, opm_bias)
    pair_one = triangle_update(pair_zero, mask_f, tri_norm[0], tri_proj[0], tri_gate[0], tri_xnorm[0], tri_out[0], False)
    return triangle_update(pair_one, mask_f, tri_norm[1], tri_proj[1], tri_gate[1], tri_xnorm[1], tri_out[1], True)
```

```python
import functools

import jax
import jax.numpy as jnp
from jax import lax
from jax.experimental import pallas as pl
from jax.experimental.pallas import tpu as pltpu
from jax.sharding import PartitionSpec as P

LN_EPS = 1e-5
F32 = jnp.float32
BF16 = jnp.bfloat16
SWAP_X = [(0, 2), (1, 3), (2, 0), (3, 1)]
SWAP_CORE = [(0, 1), (1, 0), (2, 3), (3, 2)]
NT = (((1,), (1,)), ((), ()))
TN = (((0,), (0,)), ((), ()))
VMEM_LIMIT = 60 * 1024 * 1024


def dot(lhs, rhs):
    return jnp.dot(lhs, rhs, preferred_element_type=F32)


def sigmoid(values):
    return 0.5 * jnp.tanh(0.5 * values) + 0.5


def norm_rows(values, scale, shift):
    mean = jnp.mean(values, axis=0, keepdims=True)
    centered = values - mean
    var = jnp.mean(centered * centered, axis=0, keepdims=True)
    return (centered * lax.rsqrt(var + LN_EPS) * scale + shift).astype(BF16)


def scatter_rows(scr, row, stride, values):
    for t in range(scr.shape[0]):
        scr[t, pl.ds(row, values.shape[0], stride=stride), :] = values[:, t * 128:(t + 1) * 128]


def gather_rows(scr, row, stride, count):
    return jnp.concatenate([scr[t, pl.ds(row, count, stride=stride), :] for t in range(scr.shape[0])], axis=1)


def tiled_scratch(rows, lanes):
    return pltpu.VMEM((lanes // 128, rows, 128), F32)


def flush(scr, ref):
    major, rows, _ = ref.shape
    for t in range(scr.shape[0]):
        ref[:, :, t * 128:(t + 1) * 128] = scr[t].reshape(major, rows, 128).astype(ref.dtype)


def params(n=1):
    return pltpu.CompilerParams(dimension_semantics=("arbitrary",) * n, vmem_limit_bytes=VMEM_LIMIT)


def cost(flops, nbytes):
    return pl.CostEstimate(flops=int(flops), bytes_accessed=int(nbytes), transcendentals=0)


def msa_kernel(msa_ref, norm_ref, proj_ref, left_ref, right_ref, rows_scr, right_scr):
    depth, res, dim = msa_ref.shape
    opm = proj_ref.shape[0] // 2
    vals = msa_ref[...].astype(F32)
    mean = jnp.mean(vals, axis=-1, keepdims=True)
    cent = vals - mean
    var = jnp.mean(cent * cent, axis=-1, keepdims=True)
    normed = cent * lax.rsqrt(var + LN_EPS) * norm_ref[0:1, :][None] + norm_ref[1:2, :][None]
    for t in range(dim // 128):
        rows_scr[t] = normed[:, :, t * 128:(t + 1) * 128].reshape(depth * res, 128)
    for r in range(res):
        one = gather_rows(rows_scr, r, res, depth)
        u = lax.dot_general(proj_ref[...], one.astype(BF16), NT, preferred_element_type=F32)
        left_ref[r] = u[:opm].astype(BF16)
        scatter_rows(right_scr, r, res, u[opm:])
    flush(right_scr, right_ref)


def msa_project(msa, norm, proj_t):
    depth, res, dim = msa.shape
    opm = proj_t.shape[0] // 2
    blk = 8
    return pl.pallas_call(
        msa_kernel,
        grid=(res // blk,),
        in_specs=[
            pl.BlockSpec((depth, blk, dim), lambda s: (0, s, 0)),
            pl.BlockSpec((2, dim), lambda s: (0, 0)),
            pl.BlockSpec((2 * opm, dim), lambda s: (0, 0)),
        ],
        out_specs=[
            pl.BlockSpec((blk, opm, depth), lambda s: (s, 0, 0)),
            pl.BlockSpec((opm, blk, depth), lambda s: (0, s, 0)),
        ],
        out_shape=[jax.ShapeDtypeStruct((res, opm, depth), BF16), jax.ShapeDtypeStruct((opm, res, depth), BF16)],
        scratch_shapes=[tiled_scratch(depth * blk, dim), tiled_scratch(opm * blk, depth)],
        compiler_params=params(),
        cost_estimate=cost(2e10, msa.size * 2),
        name="msa_project",
    )(msa, norm, proj_t)


def opm_kernel(left_ref, s0, s1, s2, s3, wout_ref, bias_ref, z_ref, mask_ref, norm_ref, proj_ref,
               z0_ref, a_ref, b_ref, right_scr, outer_scr, a_scr, b_scr, sem):
    me = lax.axis_index("dap")
    rb, opm, depth = left_ref.shape
    slab = s0.shape[1]
    res = right_scr.shape[1]
    chan = a_ref.shape[0]

    @pl.when(pl.program_id(0) == 0)
    def _():
        copies = []
        for t, src in enumerate((s0, s1, s2, s3)):
            off = pl.multiple_of(jnp.bitwise_xor(me, t) * slab, slab)
            copies.append(pltpu.make_async_copy(src, right_scr.at[:, pl.ds(off, slab), :], sem.at[t]))
        for cp in copies:
            cp.start()
        for cp in copies:
            cp.wait()

    left = left_ref[...].reshape(rb * opm, depth)

    def outer_step(q, _):
        o = lax.dot_general(left, right_scr[q], NT, preferred_element_type=F32) * (1.0 / depth)
        outer_scr[:, q] = o.astype(BF16).reshape(rb, opm, res)
        return 0

    lax.fori_loop(0, opm, outer_step, 0)

    def row_step(r, _):
        upd = dot(wout_ref[...], outer_scr[r].reshape(opm * opm, res)) + bias_ref[...]
        z0 = z_ref[r].T + upd
        z0_ref[r] = z0
        y = norm_rows(z0, norm_ref[:, 0:1], norm_ref[:, 1:2])
        q = dot(proj_ref[...], y)
        m = mask_ref[pl.ds(r, 1), :]
        scatter_rows(a_scr, r, rb, m * sigmoid(q[chan:2 * chan]) * q[:chan])
        scatter_rows(b_scr, r, rb, m * sigmoid(q[3 * chan:]) * q[2 * chan:3 * chan])
        return 0

    lax.fori_loop(0, rb, row_step, 0)
    flush(a_scr, a_ref)
    flush(b_scr, b_ref)


def opm_call(first, rows, left, slabs, wout_t, bias, z, mask, norm_t, proj_t, rb):
    _, opm, depth = left.shape
    slab = slabs[0].shape[1]
    res, chan = z.shape[1:]
    base = first // rb
    full = lambda shape: pl.BlockSpec(shape, lambda s: (0,) * len(shape))
    any_spec = pl.BlockSpec(memory_space=pl.ANY)
    return pl.pallas_call(
        opm_kernel,
        grid=(rows // rb,),
        in_specs=[
            pl.BlockSpec((rb, opm, depth), lambda s: (base + s, 0, 0)),
            any_spec, any_spec, any_spec, any_spec,
            full((chan, opm * opm)),
            full((chan, 1)),
            pl.BlockSpec((rb, res, chan), lambda s: (base + s, 0, 0)),
            pl.BlockSpec((rb, res), lambda s: (base + s, 0)),
            full((chan, 2)),
            full((4 * chan, chan)),
        ],
        out_specs=[
            pl.BlockSpec((rb, chan, res), lambda s: (s, 0, 0)),
            pl.BlockSpec((chan, rb, res), lambda s: (0, s, 0)),
            pl.BlockSpec((chan, rb, res), lambda s: (0, s, 0)),
        ],
        out_shape=[
            jax.ShapeDtypeStruct((rows, chan, res), F32),
            jax.ShapeDtypeStruct((chan, rows, res), BF16),
            jax.ShapeDtypeStruct((chan, rows, res), BF16),
        ],
        scratch_shapes=[
            pltpu.VMEM((opm, res, depth), BF16),
            pltpu.VMEM((rb, opm, opm, res), BF16),
            tiled_scratch(chan * rb, res),
            tiled_scratch(chan * rb, res),
            pltpu.SemaphoreType.DMA((4,)),
        ],
        compiler_params=params(),
        cost_estimate=cost(rows * 6e8, 3e7),
        name="opm",
    )(left, *slabs, wout_t, bias, z, mask, norm_t, proj_t)


def outgoing_kernel(n, *refs):
    me = lax.axis_index("dap")
    a_refs, b_refs, x_ref, a_scr, b_scr = refs[:n], refs[n:5 * n], refs[5 * n], refs[5 * n + 1], refs[5 * n + 2]
    chans = x_ref.shape[0]
    slab = x_ref.shape[1]

    def step(c, _):
        row = 0
        for ref in a_refs:
            a_scr[pl.ds(row, ref.shape[1]), :] = ref[c]
            row += ref.shape[1]
        for t in range(4):
            off = jnp.bitwise_xor(me, t) * slab
            row = 0
            for ref in b_refs[t * n:(t + 1) * n]:
                b_scr[pl.ds(pl.multiple_of(off + row, 16), ref.shape[1]), :] = ref[c]
                row += ref.shape[1]
        x_ref[c] = lax.dot_general(a_scr[...], b_scr[...], NT, preferred_element_type=F32).astype(BF16)
        return 0

    lax.fori_loop(0, chans, step, 0)


def outgoing_product(a_parts, b_parts):
    n = len(a_parts)
    chan, _, res = a_parts[0].shape
    slab = sum(p.shape[1] for p in a_parts)
    cb = 8
    ops = list(a_parts) + [p for slab_parts in b_parts for p in slab_parts]
    return pl.pallas_call(
        functools.partial(outgoing_kernel, n),
        grid=(chan // cb,),
        in_specs=[pl.BlockSpec((cb, p.shape[1], res), lambda s: (s, 0, 0)) for p in ops],
        out_specs=pl.BlockSpec((cb, slab, res), lambda s: (s, 0, 0)),
        out_shape=jax.ShapeDtypeStruct((chan, slab, res), BF16),
        scratch_shapes=[pltpu.VMEM((slab, res), BF16), pltpu.VMEM((res, res), BF16)],
        compiler_params=params(),
        cost_estimate=cost(4e9, 5.7e7),
        name="outgoing",
    )(*ops)


def update_rows(x_ref, z_ref, norm_ref, gate_ref, xnorm_ref, out_ref, x_scr, emit):
    chan, rb, res = x_ref.shape
    x = x_ref[...].astype(F32)
    mean = jnp.mean(x, axis=0, keepdims=True)
    cent = x - mean
    var = jnp.mean(cent * cent, axis=0, keepdims=True)
    normed = cent * lax.rsqrt(var + LN_EPS)
    for t in range(res // 128):
        x_scr[t] = normed[:, :, t * 128:(t + 1) * 128].reshape(chan * rb, 128)

    def row_step(r, _):
        xn = (gather_rows(x_scr, r, rb, chan) * xnorm_ref[:, 0:1] + xnorm_ref[:, 1:2]).astype(BF16)
        z = z_ref[r]
        y = norm_rows(z, norm_ref[:, 0:1], norm_ref[:, 1:2])
        g = sigmoid(dot(gate_ref[...], y))
        emit(r, z + g * dot(out_ref[...], xn))
        return 0

    lax.fori_loop(0, rb, row_step, 0)


def mid_kernel(x_ref, z_ref, norm_ref, gate_ref, xnorm_ref, out_ref, norm2_ref, z1_ref, y_ref, x_scr):
    def emit(r, z1):
        z1_ref[r] = z1
        y_ref[r] = norm_rows(z1, norm2_ref[:, 0:1], norm2_ref[:, 1:2])

    update_rows(x_ref, z_ref, norm_ref, gate_ref, xnorm_ref, out_ref, x_scr, emit)


def last_kernel(x_ref, z_ref, norm_ref, gate_ref, xnorm_ref, out_ref, z2_ref, x_scr):
    def emit(r, z2):
        z2_ref[r] = z2.T

    update_rows(x_ref, z_ref, norm_ref, gate_ref, xnorm_ref, out_ref, x_scr, emit)


def update_call(first, x, z, norm_t, gate_t, xnorm_t, out_t, norm2_t, last):
    chan, _, res = x.shape
    rows = z.shape[0]
    rb = 8
    base = first // rb
    full = lambda shape: pl.BlockSpec(shape, lambda s: (0,) * len(shape))
    row_spec = pl.BlockSpec((rb, chan, res), lambda s: (s, 0, 0))
    in_specs = [pl.BlockSpec((chan, rb, res), lambda s: (0, base + s, 0)), row_spec,
                full((chan, 2)), full((chan, chan)), full((chan, 2)), full((chan, chan))]
    ops = [x, z, norm_t, gate_t, xnorm_t, out_t]
    if last:
        out_specs = pl.BlockSpec((rb, res, chan), lambda s: (s, 0, 0))
        out_shape = jax.ShapeDtypeStruct((rows, res, chan), F32)
    else:
        in_specs.append(full((chan, 2)))
        ops.append(norm2_t)
        out_specs = [row_spec, row_spec]
        out_shape = [jax.ShapeDtypeStruct((rows, chan, res), F32), jax.ShapeDtypeStruct((rows, chan, res), BF16)]
    return pl.pallas_call(
        last_kernel if last else mid_kernel,
        grid=(rows // rb,),
        in_specs=in_specs,
        out_specs=out_specs,
        out_shape=out_shape,
        scratch_shapes=[tiled_scratch(chan * rb, res)],
        compiler_params=params(),
        cost_estimate=cost(rows * 1.5e8, 5e7),
        name="last_update" if last else "mid_update",
    )(*ops)


def incoming_kernel(n, kb, has_acc, final, *refs):
    y_refs, m_refs = refs[:n], refs[n:2 * n]
    proja_ref, projb_ref, sel_ref = refs[2 * n:2 * n + 3]
    rest = refs[2 * n + 3:]
    acc_ref = rest[0] if has_acc else None
    x_ref, a_all, b_all, a_scr, b_scr = rest[1 if has_acc else 0:]
    s = pl.program_id(0)
    cb = x_ref.shape[0]
    slab = x_ref.shape[1]
    chan, total, res = b_all.shape
    wide = a_all.shape[2]
    steps = total // kb

    per = steps // n
    for t in range(n):
        @pl.when((s >= t * per) & (s < (t + 1) * per))
        def _(y_ref=y_refs[t], m_ref=m_refs[t]):
            def row_step(r, _):
                y = y_ref[r]
                m = m_ref[pl.ds(r, 1), :]
                qb = dot(projb_ref[...], y)
                scatter_rows(b_scr, r, kb, m * sigmoid(qb[chan:]) * qb[:chan])
                ys = dot(y, sel_ref[...]).astype(BF16)
                ms = dot(m.astype(BF16), sel_ref[...])
                qa = dot(proja_ref[...], ys)
                scatter_rows(a_scr, r, kb, ms * sigmoid(qa[chan:]) * qa[:chan])
                return 0

            lax.fori_loop(0, kb, row_step, 0)
            off = pl.multiple_of(s * kb, kb)
            flush(b_scr, b_all.at[:, pl.ds(off, kb), :])
            flush(a_scr, a_all.at[:, pl.ds(off, kb), :])

    @pl.when(s >= steps)
    def _():
        def step(c, _):
            cc = (s - steps) * cb + c
            x = lax.dot_general(a_all[cc], b_all[cc], TN, preferred_element_type=F32)[:slab]
            if has_acc:
                x = x + acc_ref[c]
            x_ref[c] = x.astype(x_ref.dtype)
            return 0

        lax.fori_loop(0, cb, step, 0)


def incoming_product(y_parts, m_parts, proja_t, projb_t, sel, acc, final):
    n = len(y_parts)
    rows, chan, res = y_parts[0].shape
    slab = 96
    wide = sel.shape[1]
    kb, cb = 16, 8
    per = rows // kb
    steps = n * per
    full = lambda shape: pl.BlockSpec(shape, lambda s: (0,) * len(shape))
    clip = lambda t: (lambda s: (jnp.clip(s - t * per, 0, per - 1), 0, 0))
    clip2 = lambda t: (lambda s: (jnp.clip(s - t * per, 0, per - 1), 0))
    cspec = pl.BlockSpec((cb, slab, res), lambda s: (jnp.maximum(s - steps, 0), 0, 0))
    in_specs = [pl.BlockSpec((kb, chan, res), clip(t)) for t in range(n)]
    in_specs += [pl.BlockSpec((kb, res), clip2(t)) for t in range(n)]
    in_specs += [full((2 * chan, chan)), full((2 * chan, chan)), full((res, wide))]
    ops = list(y_parts) + list(m_parts) + [proja_t, projb_t, sel]
    if acc is not None:
        in_specs.append(cspec)
        ops.append(acc)
    return pl.pallas_call(
        functools.partial(incoming_kernel, n, kb, acc is not None, final),
        grid=(steps + chan // cb,),
        in_specs=in_specs,
        out_specs=cspec,
        out_shape=jax.ShapeDtypeStruct((chan, slab, res), BF16 if final else F32),
        scratch_shapes=[
            pltpu.VMEM((chan, n * rows, wide), BF16),
            pltpu.VMEM((chan, n * rows, res), BF16),
            tiled_scratch(chan * kb, wide),
            tiled_scratch(chan * kb, res),
        ],
        compiler_params=params(),
        cost_estimate=cost(n * rows * 1e8, 4e7),
        name="incoming",
    )(*ops)


def solution(mesh):
    row_spec = P(("data", "dap"), None, None)
    mask_spec = P(("data", "dap"), None)
    msa_spec = P(None, ("data", "dap"), None)

    def swap_x(v):
        return lax.ppermute(v, "dap", SWAP_X)

    def swap_core(v):
        return lax.ppermute(v, "dap", SWAP_CORE)

    def local_program(z, mask, msa, opm_norm, opm_proj, opm_out, opm_bias, tri_norm, tri_proj, tri_gate, tri_xnorm, tri_out):
        rows, res, chan = z.shape
        opm = opm_proj.shape[1] // 2
        me = lax.axis_index("dap")
        mask_f = mask.astype(F32)
        mask_sib = swap_core(mask_f)
        mask_cross = swap_x(mask_f)
        mask_far = swap_core(mask_cross)
        wout_t = opm_out.reshape(opm, opm, chan).transpose(2, 1, 0).reshape(chan, opm * opm)
        bias = opm_bias[:, None]
        norm_t = jnp.swapaxes(tri_norm, 1, 2)
        xnorm_t = jnp.swapaxes(tri_xnorm, 1, 2)
        proj_t = jnp.swapaxes(tri_proj, 1, 2)
        gate_t = jnp.swapaxes(tri_gate, 1, 2)
        out_t = jnp.swapaxes(tri_out, 1, 2)
        lanes = lax.broadcasted_iota(jnp.int32, (res, 128), 0)
        cols = lax.broadcasted_iota(jnp.int32, (res, 128), 1)
        sel = ((lanes == me * rows + cols) & (cols < rows)).astype(BF16)

        left, right = msa_project(msa, opm_norm, opm_proj.T)
        right_x = swap_x(right)
        slabs = [right, swap_core(right), right_x, swap_core(right_x)]

        chunk = 32
        firsts = range(0, rows, chunk)
        z0s, a_parts, b_own = [], [], []
        for first in firsts:
            z0c, ac, bc = opm_call(first, chunk, left, slabs, wout_t, bias, z, mask_f, norm_t[0], proj_t[0], 16)
            z0s.append(z0c)
            a_parts.append(ac)
            b_own.append(bc)
        b_x = [swap_x(b) for b in b_own]
        b_sib = [swap_core(b) for b in b_own]
        b_far = [swap_core(b) for b in b_x]
        x1 = outgoing_product(a_parts, [b_own, b_sib, b_x, b_far])

        z1s, ys = [], []
        for first, z0c in zip(firsts, z0s):
            z1c, yc = update_call(first, x1, z0c, norm_t[0], gate_t[0], xnorm_t[0], out_t[0], norm_t[1], False)
            z1s.append(z1c)
            ys.append(yc)
        y_x = [swap_x(v) for v in ys]
        y_sib = [swap_core(v) for v in ys]
        y_far = [swap_core(v) for v in y_x]
        m_of = lambda m: [m[f:f + chunk] for f in firsts]
        proja, projb = proj_t[1][:2 * chan], proj_t[1][2 * chan:]
        acc = incoming_product(ys + y_sib, m_of(mask_f) + m_of(mask_sib), proja, projb, sel, None, False)
        x2 = incoming_product(y_x + y_far, m_of(mask_cross) + m_of(mask_far), proja, projb, sel, acc, True)
        z1 = jnp.concatenate(z1s, 0)
        return update_call(0, x2, z1, norm_t[1], gate_t[1], xnorm_t[1], out_t[1], None, True)

    return jax.shard_map(local_program, mesh=mesh, in_specs=(row_spec, mask_spec, msa_spec) + (P(),) * 9, out_specs=row_spec, check_vma=False)
```
